128 devices in a mesh: seq: 32 (over y, z, core), dp: 4 (over x).
Axes of the slice: x: 4, y: 4, z: 4, core: 2. Of those that a mesh axis runs over, the one named last changes fastest.
Arguments:
- attention_queries: bfloat16 [32, 2, 256, 4096], P('seq', None, 'dp'), parts along dimension 2, may hold values from -5.5 to 5.5
- attention_keys: bfloat16 [32, 2, 256, 512], P('seq', None, 'dp'), parts along dimension 2, may hold values from -7.5 to 7.5
- attention_values: bfloat16 [32, 2, 256, 512], P('seq', None, 'dp'), parts along dimension 2, may hold values from -6 to 6
- attention_output: bfloat16 [32, 2, 256, 4096], P('seq', None, 'dp'), parts along dimension 2, may hold values from -6 to 6
- output_gradient: bfloat16 [32, 2, 256, 4096], P('seq', None, 'dp'), parts along dimension 2, may hold values from -48 to 48
- logsumexp_rows: float32 [32, 2, 256, 32], P('seq', None, 'dp'), parts along dimension 2, as said below
Outputs:
- grad_query: float32 [32, 2, 256, 4096], P('seq', None, 'dp'), parts along dimension 2
- key_gradient: float32 [32, 2, 256, 512], P('seq', None, 'dp'), parts along dimension 2
- value_gradient: float32 [32, 2, 256, 512], P('seq', None, 'dp'), parts along dimension 2
The draws below stay inside these ranges and needn't reach their ends.
There are 4 independent parts, one for each index of `dp`. The reference program is written for one: setup_inputs(seed, part) draws one part's arguments, and reference() takes and returns one part's arrays. A program takes and returns all parts, laid end to end along the dimension named above; each array names one. Nothing has to cross between parts.
Inputs may be any that keep to these rules, and one draw needn't show every extreme that they name: logsumexp_rows[i, h] is the logarithm of the sum over key positions t <= i of exp(scores[h, i, t]), computed from attention_queries and attention_keys in float32.
All inputs are finite; a program needn't handle non-finite values.
Results may differ from the reference program's by a relative error of at most 0.0003.
Values may be sent and summed in bfloat16 or wider, within the bound.
No kernel may reach another device: no remote copies, remote signals or barrier semaphores. Data moves between devices by JAX's collectives and lax.ppermute only.
A program may use at most 128 MiB of HBM per device.

```python
import jax
import jax.numpy as jnp
from jax import lax

HQ = 32
KEY_VALUE_HEADS = 4
HEAD_SIZE = 128
QUERY_PER_KV = 8
BLOCK_TOKENS = 64
BLOCK_PAIRS = 32


def draw_attention_queries(key, part):
    complete_shape = (BLOCK_PAIRS, 2, BLOCK_TOKENS, HQ * HEAD_SIZE)
    sampled_inputs = jnp.clip(jax.random.normal(jax.random.fold_in(key, 11), complete_shape, jnp.float32), -4.0, 4.0)
    return sampled_inputs.astype(jnp.bfloat16)


def draw_attention_keys(key, part):
    complete_shape = (BLOCK_PAIRS, 2, BLOCK_TOKENS, KEY_VALUE_HEADS, HEAD_SIZE)
    sampled_inputs = jnp.clip(jax.random.normal(jax.random.fold_in(key, 13), complete_shape, jnp.float32), -4.0, 4.0)
    sampled_inputs = sampled_inputs.reshape(BLOCK_PAIRS, 2, BLOCK_TOKENS, KEY_VALUE_HEADS * HEAD_SIZE)
    return sampled_inputs.astype(jnp.bfloat16)


def sequence_row_list(blocks):
    width = blocks.shape[-1]
    earlier_half = blocks[:, 0].reshape(BLOCK_PAIRS * BLOCK_TOKENS, width)
    later_half = blocks[::-1, 1].reshape(BLOCK_PAIRS * BLOCK_TOKENS, width)
    return jnp.concatenate([earlier_half, later_half], axis=0)


def draw_logsumexp_rows(key, part):
    sequence_length = 2 * BLOCK_PAIRS * BLOCK_TOKENS
    span_rows = 2 * BLOCK_TOKENS
    query_values_list = sequence_row_list(draw_attention_queries(key, part).astype(jnp.float32)).reshape(sequence_length, KEY_VALUE_HEADS, QUERY_PER_KV, HEAD_SIZE)
    every_key = sequence_row_list(draw_attention_keys(key, part).astype(jnp.float32)).reshape(sequence_length, KEY_VALUE_HEADS, HEAD_SIZE)
    key_pos = jnp.arange(sequence_length, dtype=jnp.int32)

    def per_block(block_index):
        first_row = (block_index * span_rows).astype(jnp.int32)
        query_blk = lax.dynamic_slice_in_dim(query_values_list, first_row, span_rows, 0)
        query_pos = first_row + jnp.arange(span_rows, dtype=jnp.int32)
        allowed = key_pos[None, :] <= query_pos[:, None]
        scores = HEAD_SIZE ** (-0.5) * jnp.einsum('qhgd,khd->hgqk', query_blk, every_key, precision=lax.Precision.HIGHEST)
        largest = jnp.max(jnp.where(allowed, scores, -1e+30), axis=-1, keepdims=True)
        expsum = jnp.sum(jnp.where(allowed, jnp.exp(scores - largest), 0.0), axis=-1, keepdims=True)
        totals = (largest + jnp.log(expsum))[..., 0]
        return totals.transpose(2, 0, 1).reshape(span_rows, HQ)
    rows_all = lax.map(per_block, jnp.arange(BLOCK_PAIRS, dtype=jnp.int32)).reshape(sequence_length, HQ)
    earlier_half = rows_all[:BLOCK_PAIRS * BLOCK_TOKENS].reshape(BLOCK_PAIRS, BLOCK_TOKENS, HQ)
    later_half = rows_all[BLOCK_PAIRS * BLOCK_TOKENS:].reshape(BLOCK_PAIRS, BLOCK_TOKENS, HQ)[::-1]
    return jnp.stack([earlier_half, later_half], axis=1).astype(jnp.float32)


def shard_levels(key, extent, cuts, least, high):
    gain = 1.0
    for position, shards_of in cuts:
        draws = jax.random.uniform(jax.random.fold_in(jax.random.fold_in(key, 6), position), (shards_of,), jnp.float32, least / len(cuts), high / len(cuts))
        gain = gain * jnp.repeat(jnp.exp(draws), extent[position] // shards_of).reshape((-1,) + (1,) * (len(extent) - 1 - position))
    return gain


def gaussian(key, extent, deviation, bound, cuts=(), held_as=jnp.bfloat16):
    values = jax.random.normal(key, extent, jnp.float32) * deviation
    if len(cuts) > 0:
        values = shard_levels(key, extent, cuts, -0.22, 0.18) * values
    return jnp.clip(values, min=-bound, max=bound).astype(held_as)


def setup_inputs(seed: int = 0, part: int = 0) -> dict:
    streams_of = jax.random.split(jax.random.key(seed), 7)
    part_splits = jax.random.split(jax.random.fold_in(streams_of[6], part), 7)
    return {
        "attention_queries": draw_attention_queries(jax.random.fold_in(jax.random.fold_in(streams_of[6], part), 71), part),
        "attention_keys": draw_attention_keys(jax.random.fold_in(jax.random.fold_in(streams_of[6], part), 71), part),
        "attention_values": gaussian(part_splits[2], (BLOCK_PAIRS, 2, BLOCK_TOKENS, KEY_VALUE_HEADS * HEAD_SIZE), 1.0, 6.0, ((0, 32),)),
        "attention_output": gaussian(part_splits[3], (BLOCK_PAIRS, 2, BLOCK_TOKENS, HQ * HEAD_SIZE), 1.0, 6.0, ((0, 32),)),
        "output_gradient": gaussian(part_splits[4], (BLOCK_PAIRS, 2, BLOCK_TOKENS, HQ * HEAD_SIZE), 8.0, 48.0, ((0, 32),)),
        "logsumexp_rows": draw_logsumexp_rows(jax.random.fold_in(jax.random.fold_in(streams_of[6], part), 71), part),
    }


def blocks_to_sequence(blocks):
    earlier_half = blocks[:, 0].reshape(BLOCK_PAIRS * BLOCK_TOKENS, blocks.shape[-1])
    later_half = blocks[::-1, 1].reshape(BLOCK_PAIRS * BLOCK_TOKENS, blocks.shape[-1])
    return jnp.concatenate([earlier_half, later_half], axis=0)


def to_blocks(sequence):
    earlier_half = sequence[: BLOCK_PAIRS * BLOCK_TOKENS].reshape(BLOCK_PAIRS, BLOCK_TOKENS, sequence.shape[-1])
    later_half = sequence[BLOCK_PAIRS * BLOCK_TOKENS:].reshape(BLOCK_PAIRS, BLOCK_TOKENS, sequence.shape[-1])[::-1]
    return jnp.stack([earlier_half, later_half], axis=1)


def split_low(values):
    high_part = values.astype(jnp.bfloat16)
    back_value = lax.optimization_barrier(high_part).astype(jnp.float32)
    rest_part = (values - back_value).astype(jnp.bfloat16)
    return high_part.astype(jnp.float32), rest_part.astype(jnp.float32)


def reference(attention_queries, attention_keys, attention_values, attention_output, output_gradient, logsumexp_rows):
    scaling = HEAD_SIZE ** -0.5
    sequence_length = 2 * BLOCK_PAIRS * BLOCK_TOKENS
    span_rows = 2 * BLOCK_TOKENS
    query_values_list = blocks_to_sequence(attention_queries).reshape(sequence_length, KEY_VALUE_HEADS, QUERY_PER_KV, HEAD_SIZE)
    gradient_sequence = blocks_to_sequence(output_gradient).reshape(sequence_length, KEY_VALUE_HEADS, QUERY_PER_KV, HEAD_SIZE)
    output_sequence = blocks_to_sequence(attention_output).reshape(sequence_length, KEY_VALUE_HEADS, QUERY_PER_KV, HEAD_SIZE)
    logsum_sequence = blocks_to_sequence(logsumexp_rows).reshape(sequence_length, KEY_VALUE_HEADS, QUERY_PER_KV)
    key_as_float = blocks_to_sequence(attention_keys).reshape(sequence_length, KEY_VALUE_HEADS, HEAD_SIZE).astype(jnp.float32)
    value_as_float = blocks_to_sequence(attention_values).reshape(sequence_length, KEY_VALUE_HEADS, HEAD_SIZE).astype(jnp.float32)
    key_pos = jnp.arange(sequence_length, dtype=jnp.int32)

    def per_block(carried, block_index):
        grad_keys, grad_values = carried
        first_row = (block_index * span_rows).astype(jnp.int32)
        query_blk = lax.dynamic_slice_in_dim(query_values_list, first_row, span_rows, 0).astype(jnp.float32)
        grad_blk = lax.dynamic_slice_in_dim(gradient_sequence, first_row, span_rows, 0).astype(jnp.float32)
        output_blk = lax.dynamic_slice_in_dim(output_sequence, first_row, span_rows, 0).astype(jnp.float32)
        log_blk = lax.dynamic_slice_in_dim(logsum_sequence, first_row, span_rows, 0).transpose(1, 2, 0)[..., None]
        query_pos = first_row + jnp.arange(span_rows, dtype=jnp.int32)
        allowed = key_pos[None, :] <= query_pos[:, None]
        scores = scaling * jnp.einsum("qhgd,khd->hgqk", query_blk, key_as_float)
        weights = jnp.where(allowed, jnp.exp(scores - log_blk), 0.0)
        weights_high, weights_rest = split_low(weights)
        row_delta = jnp.sum(grad_blk * output_blk, axis=-1)
        weight_grad = jnp.einsum("qhgd,khd->hgqk", grad_blk, value_as_float)
        score_grad = weights * (weight_grad - row_delta.transpose(1, 2, 0)[..., None])
        score_high, score_rest = split_low(score_grad)
        grad_values = grad_values + jnp.einsum("hgqk,qhgd->khd", weights_high, grad_blk) + jnp.einsum("hgqk,qhgd->khd", weights_rest, grad_blk)
        grad_keys = grad_keys + scaling * (jnp.einsum("hgqk,qhgd->khd", score_high, query_blk) + jnp.einsum("hgqk,qhgd->khd", score_rest, query_blk))
        grad_query = scaling * (jnp.einsum("hgqk,khd->qhgd", score_high, key_as_float) + jnp.einsum("hgqk,khd->qhgd", score_rest, key_as_float))
        return (grad_keys, grad_values), grad_query

    zero_key_value = jnp.zeros((sequence_length, KEY_VALUE_HEADS, HEAD_SIZE), jnp.float32)
    final_results, grad_blocks = lax.scan(per_block, (zero_key_value, zero_key_value), jnp.arange(BLOCK_PAIRS, dtype=jnp.int32))
    grad_query = grad_blocks.reshape(sequence_length, HQ * HEAD_SIZE)
    key_gradient = final_results[0].reshape(sequence_length, KEY_VALUE_HEADS * HEAD_SIZE)
    value_gradient = final_results[1].reshape(sequence_length, KEY_VALUE_HEADS * HEAD_SIZE)
    return to_blocks(grad_query), to_blocks(key_gradient), to_blocks(value_gradient)
```

```python
import jax
import jax.numpy as jnp
from jax import lax
from jax.experimental import pallas as pl
from jax.experimental.pallas import tpu as pltpu
from jax.sharding import PartitionSpec as P

HEAD = 128
GROUP = 8
BLOCK = 64
ROWS = GROUP * BLOCK
WIDTH = GROUP * HEAD
HEADS = 4
TILE = 512
SCALE = HEAD ** -0.5
LOG2E = 1.4426950408889634
F32 = jnp.float32
BF16 = jnp.bfloat16


def along_y(step):
    return [(i, (i + 8 * step) % 32) for i in range(32)]


def along_z(step):
    return [(i, (i // 8) * 8 + (i + 2 * step) % 8) for i in range(32)]


OTHER_CORE = [(i, i ^ 1) for i in range(32)]
Y_GROUPS = [[zc + 8 * y for y in range(4)] for zc in range(8)]


def three_way(values):
    high = lax.reduce_precision(values, 8, 7)
    left = values - high
    middle = lax.reduce_precision(left, 8, 7)
    return high.astype(BF16), middle.astype(BF16), (left - middle).astype(BF16)


def dot(a, b):
    return jnp.dot(a, b, preferred_element_type=F32)


def split(values):
    high = values.astype(BF16)
    return high, (values - high.astype(F32)).astype(BF16)


def attention_kernel(
    place_ref, x0, x1, x2, x3, kv_own, kv_other, dq_ref, own_ref, other_ref,
    k_s, kt_s, v_s, dk_s, dv_s, qt_s, dot_s, q_s, do_s, dqt_s, aux_s,
):
    step = pl.program_id(0)
    y, z, c = place_ref[0], place_ref[1], place_ref[2]
    pair = step // 2
    half = step % 2
    owner = ((y + place_ref[3 + pair]) % 4) * 8 + z * 2 + c
    block = jnp.where(half == 0, owner, 63 - owner)

    def rows_of(slot_z, slot_y, core, a):
        n = slot_y * 8 + slot_z * 2 + core
        return pl.ds(pl.multiple_of((n if a == 0 else 63 - n) * BLOCK, BLOCK), BLOCK)

    @pl.when(step == 0)
    def _():
        dk_s[...] = jnp.zeros_like(dk_s)
        dv_s[...] = jnp.zeros_like(dv_s)
        for ref, core in ((kv_own, c), (kv_other, 1 - c)):
            for k in range(4):
                for s in range(4):
                    for a in range(2):
                        rows = rows_of((z - k + 4) % 4, s, core, a)
                        k_s[rows, :] = ref[k, s, 0, a]
                        v_s[rows, :] = ref[k, s, 1, a]
        kt_s[...] = k_s[...].T

    def take(x_ref):
        for j in range(GROUP):
            q = x_ref[half, 0:BLOCK, j * HEAD:(j + 1) * HEAD]
            d = x_ref[half, 0:BLOCK, WIDTH + j * HEAD:WIDTH + (j + 1) * HEAD]
            for at in (0, ROWS):
                q_s[at + j * BLOCK:at + (j + 1) * BLOCK, :] = q
                do_s[at + j * BLOCK:at + (j + 1) * BLOCK, :] = d
        aux = x_ref[half, BLOCK:BLOCK + 16, :].astype(F32)
        logs = aux[0:1, 0:512] + aux[0:1, 512:1024] + aux[0:1, 1024:1536]
        aux_s[0:1, :] = logs * LOG2E
        aux_s[1:2, :] = aux[0:1, 1536:2048] + aux[1:2, 0:512] + aux[1:2, 512:1024]

    for p, x_ref in enumerate((x0, x1, x2, x3)):
        pl.when(pair == p)(lambda x_ref=x_ref: take(x_ref))
    qt_s[...] = q_s[0:ROWS, :].T
    dot_s[...] = do_s[0:ROWS, :].T
    dqt_s[...] = jnp.zeros_like(dqt_s)

    def tile(t, masked):
        at = pl.multiple_of(t * TILE, TILE)
        keys = pl.ds(at, TILE)
        scores = dot(k_s[keys, :], qt_s[...])
        weight_grad = dot(v_s[keys, :], dot_s[...])
        weights = jnp.exp2(scores * (SCALE * LOG2E) - aux_s[0:1, :])
        if masked:
            key_pos = at + lax.broadcasted_iota(jnp.int32, (TILE, ROWS), 0)
            within = lax.broadcasted_iota(jnp.int32, (TILE, ROWS), 1) % BLOCK
            weights = jnp.where(key_pos <= block * BLOCK + within, weights, 0.0)
        w_high, w_rest = split(weights)
        s_high, s_rest = split(weights * (weight_grad - aux_s[1:2, :]))
        dv_s[keys, :] += dot(jnp.concatenate([w_high, w_rest], 1), do_s[...])
        dk_s[keys, :] += dot(jnp.concatenate([s_high, s_rest], 1), q_s[...])
        kt = kt_s[:, keys]
        dqt_s[...] += dot(
            jnp.concatenate([kt, kt], 1), jnp.concatenate([s_high, s_rest], 0)
        )

    full = (block * BLOCK) // TILE

    @pl.loop(0, full)
    def _(t):
        tile(t, False)

    tile(full, True)
    dq = (dqt_s[...] * SCALE).T
    for j in range(GROUP):
        dq_ref[0, 0, :, j * HEAD:(j + 1) * HEAD] = dq[j * BLOCK:(j + 1) * BLOCK, :]

    @pl.when(step == 7)
    def _():
        for ref, core in ((own_ref, c), (other_ref, 1 - c)):
            for k in range(4):
                for s in range(4):
                    for a in range(2):
                        rows = rows_of((z + k) % 4, s, core, a)
                        ref[k, s, 0, a] = dk_s[rows, :] * SCALE
                        ref[k, s, 1, a] = dv_s[rows, :]


def attention(place, xs, kv_own, kv_other):
    whole = lambda shape: pl.BlockSpec(shape, lambda i, p: (0,) * len(shape))
    keys = 64 * BLOCK
    kv_shape = (4, 4, 2, 2, BLOCK, HEAD)
    return pl.pallas_call(
        attention_kernel,
        grid_spec=pltpu.PrefetchScalarGridSpec(
            num_scalar_prefetch=1,
            grid=(8,),
            in_specs=[whole((2, BLOCK + 16, 2 * WIDTH))] * 4 + [whole(kv_shape)] * 2,
            out_specs=[
                pl.BlockSpec((1, 1, BLOCK, WIDTH), lambda i, p: (i // 2, i % 2, 0, 0)),
                whole(kv_shape),
                whole(kv_shape),
            ],
            scratch_shapes=[
                pltpu.VMEM((keys, HEAD), BF16),
                pltpu.VMEM((HEAD, keys), BF16),
                pltpu.VMEM((keys, HEAD), BF16),
                pltpu.VMEM((keys, HEAD), F32),
                pltpu.VMEM((keys, HEAD), F32),
                pltpu.VMEM((HEAD, ROWS), BF16),
                pltpu.VMEM((HEAD, ROWS), BF16),
                pltpu.VMEM((2 * ROWS, HEAD), BF16),
                pltpu.VMEM((2 * ROWS, HEAD), BF16),
                pltpu.VMEM((HEAD, ROWS), F32),
                pltpu.VMEM((8, ROWS), F32),
            ],
        ),
        out_shape=[
            jax.ShapeDtypeStruct((4, 2, BLOCK, WIDTH), F32),
            jax.ShapeDtypeStruct(kv_shape, F32),
            jax.ShapeDtypeStruct(kv_shape, F32),
        ],
        compiler_params=pltpu.CompilerParams(
            dimension_semantics=("arbitrary",), vmem_limit_bytes=60 * 2**20
        ),
        name="attention_backward",
    )(place, *xs, kv_own, kv_other)


def body(queries, keys, values, output, output_grad, logs):
    index = lax.axis_index("seq").astype(jnp.int32)
    y, z, c = index // 8, (index // 2) % 4, index % 2
    send = lambda a, perm: lax.ppermute(a, "seq", perm)

    def kv_heads(a):
        return a[0].reshape(2, BLOCK, HEADS, HEAD).transpose(2, 0, 1, 3)

    kv = jnp.stack([kv_heads(keys), kv_heads(values)], 1)
    kv = lax.all_to_all(kv, "seq", 0, 0, axis_index_groups=Y_GROUPS, tiled=True)

    delta = jnp.sum(
        (output_grad[0].astype(F32) * output[0].astype(F32)).reshape(
            2, BLOCK, HEADS, GROUP, HEAD
        ),
        -1,
    )

    def aux_rows(a):
        return a.transpose(2, 0, 3, 1).reshape(HEADS, 2, 1, ROWS)

    log_parts = three_way(aux_rows(logs[0].reshape(2, BLOCK, HEADS, GROUP)))
    delta_parts = three_way(aux_rows(delta))
    nothing = jnp.zeros((HEADS, 2, 1, ROWS), BF16)
    first = jnp.concatenate([*log_parts, delta_parts[0]], -1)
    second = jnp.concatenate([delta_parts[1], delta_parts[2], nothing, nothing], -1)
    aux = jnp.concatenate(
        [first, second, jnp.zeros((HEADS, 2, 14, 4 * ROWS), BF16)], 2
    )

    def payload(head):
        start = head * WIDTH
        q = lax.dynamic_slice_in_dim(queries[0], start, WIDTH, 2)
        d = lax.dynamic_slice_in_dim(output_grad[0], start, WIDTH, 2)
        a = lax.dynamic_index_in_dim(aux, head, 0, False)
        return jnp.concatenate([jnp.concatenate([q, d], -1), a], 1)

    steps = (0, 1, 3, 2)
    xs = [payload(y)] + [send(payload((y + k) % 4), along_y(k)) for k in steps[1:]]
    kv_own = jnp.stack([kv] + [send(kv, along_z(k)) for k in (1, 2, 3)])
    kv_other = send(kv_own, OTHER_CORE)

    place = jnp.stack([y, z, c] + [jnp.int32(-k % 4) for k in steps])
    dq, own, other = attention(place, xs, kv_own, kv_other)

    grad_query = jnp.zeros((2, BLOCK, HEADS * WIDTH), F32)
    for p, k in enumerate(steps):
        back = dq[p] if k == 0 else send(dq[p], along_y(-k))
        grad_query = lax.dynamic_update_slice_in_dim(
            grad_query, back, ((y + k) % 4) * WIDTH, 2
        )

    total = own + send(other, OTHER_CORE)
    mine = total[0]
    for k in (1, 2, 3):
        mine = mine + send(total[k], along_z(k))
    mine = lax.all_to_all(mine, "seq", 0, 0, axis_index_groups=Y_GROUPS, tiled=True)

    def tokens(a):
        return a.transpose(1, 2, 0, 3).reshape(1, 2, BLOCK, HEADS * HEAD)

    return grad_query[None], tokens(mine[:, 0]), tokens(mine[:, 1])


def solution(mesh):
    placed = P("seq", None, "dp", None)
    return jax.shard_map(
        body,
        mesh=mesh,
        in_specs=(placed,) * 6,
        out_specs=(placed,) * 3,
        check_vma=False,
    )
```

```python
import jax
import jax.numpy as jnp
from jax import lax
from jax.experimental import pallas as pl
from jax.experimental.pallas import tpu as pltpu
from jax.sharding import PartitionSpec as P

HEAD = 128
GROUP = 8
BLOCK = 64
ROWS = GROUP * BLOCK
WIDTH = GROUP * HEAD
HEADS = 4
TILE = 512
VMEM_LIMIT = 28 * 2**20
HALF = 32 * BLOCK
STEPS = (0, 1, 3, 2)
SCALE = HEAD ** -0.5
LOG2E = 1.4426950408889634
F32 = jnp.float32
BF16 = jnp.bfloat16


def along_y(step):
    return [(i, (i + 8 * step) % 32) for i in range(32)]


def along_z(step):
    return [(i, (i // 8) * 8 + (i + 2 * step) % 8) for i in range(32)]


OTHER_CORE = [(i, i ^ 1) for i in range(32)]
Y_GROUPS = [[zc + 8 * y for y in range(4)] for zc in range(8)]


def dot(a, b):
    return jnp.dot(a, b, preferred_element_type=F32)


def split(values):
    high = values.astype(BF16)
    return high, (values - high.astype(F32)).astype(BF16)


def owner_of(index, back):
    y, z, c = index // 8, (index // 2) % 4, index % 2
    return ((y + 4 - back) % 4) * 8 + z * 2 + c


def load_block(x_ref, work):
    q_s, do_s, qt_s, dot_s, log_s, delta_s = work
    for j in range(GROUP):
        q_s[j * BLOCK:(j + 1) * BLOCK, :] = x_ref[0, 0:BLOCK, j * HEAD:(j + 1) * HEAD]
        do_s[j * BLOCK:(j + 1) * BLOCK, :] = x_ref[
            0, 0:BLOCK, WIDTH + j * HEAD:WIDTH + (j + 1) * HEAD
        ]
    qt, dt = q_s[...].T, do_s[...].T
    for at in (0, ROWS):
        qt_s[:, at:at + ROWS] = qt
        dot_s[:, at:at + ROWS] = dt
    aux = x_ref[0, :, 2 * WIDTH:].astype(F32)
    aux = aux[:, 0:16] + aux[:, 16:32] + aux[:, 32:48]
    for j in range(GROUP):
        rows = slice(j * BLOCK, (j + 1) * BLOCK)
        log_s[rows, :] = jnp.broadcast_to(aux[:, j:j + 1] * LOG2E, (BLOCK, HEAD))
        delta_s[rows, :] = jnp.broadcast_to(
            aux[:, GROUP + j:GROUP + j + 1], (BLOCK, HEAD)
        )


def sweep(block, low, high, masked, base, kt_ref, vt_ref, dk_ref, dv_ref, dq_s, work, rel_s):
    q_s, do_s, qt_s, dot_s, log_s, delta_s = work
    repeat = TILE // HEAD

    def tile(t, diagonal):
        at = pl.multiple_of(t * TILE - base, TILE)
        keys = pl.ds(at, TILE)
        kt, vt = kt_ref[:, keys], vt_ref[:, keys]
        scores = dot(q_s[...], kt)
        weight_grad = dot(do_s[...], vt)
        log_b = jnp.concatenate([log_s[...]] * repeat, 1)
        delta_b = jnp.concatenate([delta_s[...]] * repeat, 1)
        weights = jnp.exp2(scores * (SCALE * LOG2E) - log_b)
        if diagonal:
            weights = jnp.where(rel_s[...] <= block * BLOCK - t * TILE, weights, 0.0)
        w_high, w_rest = split(weights)
        s_high, s_rest = split(weights * (weight_grad - delta_b))
        dv_ref[:, keys] += dot(dot_s[...], jnp.concatenate([w_high, w_rest], 0))
        dk_ref[:, keys] += dot(qt_s[...], jnp.concatenate([s_high, s_rest], 0))
        dq_s[...] += dot(
            jnp.concatenate([kt, kt], 1), jnp.concatenate([s_high.T, s_rest.T], 0)
        )

    @pl.loop(low, high)
    def _(t):
        tile(t, False)

    if masked is True:
        tile(high, True)
    elif masked is not False:
        @pl.when(masked)
        def _():
            tile(high, True)


def relative(rel_s):
    shape = (ROWS, TILE)
    rel_s[...] = lax.broadcasted_iota(jnp.int32, shape, 1) - (
        lax.broadcasted_iota(jnp.int32, shape, 0) % BLOCK
    )


def write_queries(dq_s, dq_ref):
    dq = (dq_s[...] * SCALE).T
    for j in range(GROUP):
        dq_ref[0, :, j * HEAD:(j + 1) * HEAD] = dq[j * BLOCK:(j + 1) * BLOCK, :]


def write_slots(index, late, dk_s, dv_s, out_s, own_ref, other_ref):
    z, c = (index // 2) % 4, index % 2
    for kind, acc in ((0, dk_s), (1, dv_s)):
        out_s[...] = (acc[...] * SCALE).T if kind == 0 else acc[...].T
        for ref, core in ((own_ref, c), (other_ref, 1 - c)):
            for k in range(4):
                for s in range(4):
                    n = s * 8 + ((z + k) % 4) * 2 + core
                    row = (31 - n if late else n) * BLOCK
                    rows = pl.ds(pl.multiple_of(row, BLOCK), BLOCK)
                    ref[k, s, kind] = out_s[rows, :]


def own_kernel(
    index_ref, x_ref, kv_own, kv_other, dq_ref, kt_ref, vt_ref, dk_ref, dv_ref,
    *scratch,
):
    k_s, v_s, dq_s, rel_s, *work = scratch
    half = pl.program_id(0)
    index = index_ref[0]
    y, z, c = index // 8, (index // 2) % 4, index % 2
    owner = owner_of(index, 0)
    block = jnp.where(half == 0, owner, 63 - owner)

    @pl.when(half == 0)
    def _():
        relative(rel_s)
        dk_ref[...] = jnp.zeros_like(dk_ref)
        dv_ref[...] = jnp.zeros_like(dv_ref)
        for ref, core in ((kv_own, c), (kv_other, 1 - c)):
            for k in range(4):
                for s in range(4):
                    n = ((y + 4 - STEPS[s]) % 4) * 8 + ((z - k + 4) % 4) * 2 + core
                    for a in range(2):
                        row = (n if a == 0 else 63 - n) * BLOCK
                        rows = pl.ds(pl.multiple_of(row, BLOCK), BLOCK)
                        k_s[rows, :] = ref[k, s, 0, a]
                        v_s[rows, :] = ref[k, s, 1, a]
        kt_ref[...] = k_s[...].T
        vt_ref[...] = v_s[...].T

    load_block(x_ref, work)
    dq_s[...] = jnp.zeros_like(dq_s)
    full = block // (TILE // BLOCK)
    sweep(block, 0, full, True, 0, kt_ref, vt_ref, dk_ref, dv_ref, dq_s, work, rel_s)
    write_queries(dq_s, dq_ref)


def late_kernel(
    index_ref, x1, x2, x3, kt_ref, vt_ref, dk_in, dv_in, dq_ref, own_ref, other_ref,
    *scratch,
):
    dk_s, dv_s, out_s, dq_s, rel_s, *work = scratch
    step = pl.program_id(0)
    index = index_ref[0]

    @pl.when(step == 0)
    def _():
        relative(rel_s)
        dk_s[...] = dk_in[...]
        dv_s[...] = dv_in[...]

    for p, x_ref in enumerate((x1, x2, x3)):
        pl.when(step == p)(lambda x_ref=x_ref: load_block(x_ref, work))
    back = jnp.where(step == 0, STEPS[1], jnp.where(step == 1, STEPS[2], STEPS[3]))
    block = 63 - owner_of(index, back)
    dq_s[...] = jnp.zeros_like(dq_s)
    full = block // (TILE // BLOCK)
    sweep(
        block, HALF // TILE, full, True, HALF, kt_ref, vt_ref, dk_s, dv_s, dq_s, work,
        rel_s,
    )
    dq_ref[0] = dq_s[...]

    @pl.when(step == 2)
    def _():
        write_slots(index, True, dk_s, dv_s, out_s, own_ref, other_ref)


def early_kernel(pairs, last, index_ref, *refs):
    count = len(pairs)
    x_refs, refs = refs[:count], refs[count:]
    kt_ref, vt_ref, dk_in, dv_in, dq_in, dq_ref, *rest = refs
    if last:
        own_ref, other_ref, dk_s, dv_s, out_s, dq_s, rel_s, *work = rest
    else:
        dk_s, dv_s, dq_s, rel_s, *work = rest
    step = pl.program_id(0)
    index = index_ref[0]
    back = STEPS[pairs[0]]
    if count == 2:
        back = jnp.where(step < 2, back, STEPS[pairs[1]])
    owner = owner_of(index, back)
    first = step % 2 == 0
    block = jnp.where(first, 63 - owner, owner)

    @pl.when(step == 0)
    def _():
        relative(rel_s)
        dk_s[...] = dk_in[...]
        dv_s[...] = dv_in[...]

    @pl.when(first)
    def _():
        dq_s[...] = dq_in[0]

    @pl.when(step % 2 == 1)
    def _():
        dq_s[...] = jnp.zeros_like(dq_s)

    if count == 1:
        load_block(x_refs[0], work)
    else:
        for p, x_ref in enumerate(x_refs):
            pl.when(step // 2 == p)(lambda x_ref=x_ref: load_block(x_ref, work))
    full = jnp.minimum(block // (TILE // BLOCK), HALF // TILE)
    sweep(
        block, 0, full, step % 2 == 1, 0, kt_ref, vt_ref, dk_s, dv_s, dq_s, work, rel_s
    )
    write_queries(dq_s, dq_ref)

    if last:
        @pl.when(step == 2 * count - 1)
        def _():
            write_slots(index, False, dk_s, dv_s, out_s, own_ref, other_ref)


WORK = [
    pltpu.VMEM((HEAD, ROWS), F32),
    pltpu.VMEM((ROWS, TILE), jnp.int32),
    pltpu.VMEM((ROWS, HEAD), BF16),
    pltpu.VMEM((ROWS, HEAD), BF16),
    pltpu.VMEM((HEAD, 2 * ROWS), BF16),
    pltpu.VMEM((HEAD, 2 * ROWS), BF16),
    pltpu.VMEM((ROWS, HEAD), F32),
    pltpu.VMEM((ROWS, HEAD), F32),
]
PACKED = 2 * WIDTH + HEAD
X_BLOCK = (1, BLOCK, PACKED)
SLOTS = (4, 4, 2, BLOCK, HEAD)


def whole(shape):
    return pl.BlockSpec(shape, lambda i, p: (0,) * len(shape))


def half_of(which):
    return pl.BlockSpec((HEAD, HALF), lambda i, p: (0, which))


def call(kernel, steps, ins, outs, scratch, micros):
    return pl.pallas_call(
        kernel,
        grid_spec=pltpu.PrefetchScalarGridSpec(
            num_scalar_prefetch=1,
            grid=(steps,),
            in_specs=ins,
            out_specs=[spec for spec, _ in outs],
            scratch_shapes=scratch,
        ),
        out_shape=[shape for _, shape in outs],
        compiler_params=pltpu.CompilerParams(
            dimension_semantics=("arbitrary",), vmem_limit_bytes=VMEM_LIMIT
        ),
        cost_estimate=pl.CostEstimate(
            flops=int(micros * 5e8), transcendentals=0, bytes_accessed=8 * 2**20
        ),
    )


DQ_BLOCK = (1, BLOCK, WIDTH)


def own_call(index, x, kv_own, kv_other):
    keys = 2 * HALF
    kv_shape = (4, 4, 2, 2, BLOCK, HEAD)
    return call(
        own_kernel,
        2,
        [pl.BlockSpec(X_BLOCK, lambda i, p: (i, 0, 0)), whole(kv_shape), whole(kv_shape)],
        [
            (
                pl.BlockSpec(DQ_BLOCK, lambda i, p: (i, 0, 0)),
                jax.ShapeDtypeStruct((2, BLOCK, WIDTH), F32),
            ),
            (whole((HEAD, keys)), jax.ShapeDtypeStruct((HEAD, keys), BF16)),
            (whole((HEAD, keys)), jax.ShapeDtypeStruct((HEAD, keys), BF16)),
            (whole((HEAD, keys)), jax.ShapeDtypeStruct((HEAD, keys), F32)),
            (whole((HEAD, keys)), jax.ShapeDtypeStruct((HEAD, keys), F32)),
        ],
        [pltpu.VMEM((keys, HEAD), BF16)] * 2 + WORK,
        13,
    )(index, x, kv_own, kv_other)


SLOT_OUTS = [(whole(SLOTS), jax.ShapeDtypeStruct(SLOTS, F32))] * 2
ACCUMULATORS = [pltpu.VMEM((HEAD, HALF), F32)] * 2
TURNED = [pltpu.VMEM((HALF, HEAD), F32)]


def late_call(index, xs, kt, vt, dk, dv):
    return call(
        late_kernel,
        3,
        [pl.BlockSpec(X_BLOCK, lambda i, p: (1, 0, 0))] * 3 + [half_of(1)] * 4,
        [
            (
                pl.BlockSpec((1, HEAD, ROWS), lambda i, p: (i, 0, 0)),
                jax.ShapeDtypeStruct((3, HEAD, ROWS), F32),
            )
        ] + SLOT_OUTS,
        ACCUMULATORS + TURNED + WORK,
        10,
    )(index, *xs, kt, vt, dk, dv)


def early_call(pairs, index, xs, kt, vt, dk, dv, dq):
    count, last = len(pairs), pairs[-1] == 3
    acc = [(whole((HEAD, HALF)), jax.ShapeDtypeStruct((HEAD, HALF), F32))] * 2
    return call(
        lambda *refs: early_kernel(pairs, last, *refs),
        2 * count,
        [pl.BlockSpec(X_BLOCK, lambda i, p: (1 - i % 2, 0, 0))] * count
        + [half_of(0)] * 4
        + [pl.BlockSpec((1, HEAD, ROWS), lambda i, p: (pairs[0] - 1 + i // 2, 0, 0))],
        [
            (
                pl.BlockSpec(DQ_BLOCK, lambda i, p: ((i // 2) * 2 + 1 - i % 2, 0, 0)),
                jax.ShapeDtypeStruct((2 * count, BLOCK, WIDTH), F32),
            )
        ] + (SLOT_OUTS if last else acc),
        (ACCUMULATORS + TURNED if last else []) + WORK,
        9 * count,
    )(index, *[xs[p] for p in pairs], kt, vt, dk, dv, dq)


def kv_pack_kernel(index_ref, k_ref, v_ref, *outs):
    y = index_ref[0] // 8
    for p, out in enumerate(outs):
        at = pl.multiple_of(((y + STEPS[p]) % 4) * HEAD, HEAD)
        out[0] = k_ref[0, :, :, pl.ds(at, HEAD)]
        out[1] = v_ref[0, :, :, pl.ds(at, HEAD)]


def kv_pack(index, keys, values):
    shape = (2, 2, BLOCK, HEAD)
    return call(
        kv_pack_kernel,
        1,
        [whole(keys.shape)] * 2,
        [(whole(shape), jax.ShapeDtypeStruct(shape, BF16))] * 4,
        [],
        1,
    )(index, keys, values)


def x_pack_kernel(index_ref, q_ref, d_ref, o_ref, log_ref, *outs):
    y = index_ref[0] // 8
    for p, out in enumerate(outs):
        head = (y + STEPS[p]) % 4
        at = pl.multiple_of(head * WIDTH, WIDTH)
        for a in range(2):
            q = q_ref[0, a, :, pl.ds(at, WIDTH)]
            d = d_ref[0, a, :, pl.ds(at, WIDTH)]
            o = o_ref[0, a, :, pl.ds(at, WIDTH)]
            out[a, :, 0:WIDTH] = q
            out[a, :, WIDTH:2 * WIDTH] = d
            product = d.astype(F32) * o.astype(F32)
            logs = log_ref[0, a]
            mine = logs[:, 0:GROUP]
            for h in range(1, HEADS):
                mine = jnp.where(head == h, logs[:, h * GROUP:(h + 1) * GROUP], mine)
            rows = jnp.concatenate(
                [mine]
                + [
                    jnp.sum(product[:, j * HEAD:(j + 1) * HEAD], 1, keepdims=True)
                    for j in range(GROUP)
                ],
                1,
            )
            high = rows.astype(BF16).astype(F32)
            middle = (rows - high).astype(BF16).astype(F32)
            low = rows - high - middle
            nothing = jnp.zeros((BLOCK, HEAD - 48), F32)
            out[a, :, 2 * WIDTH:] = jnp.concatenate(
                [high, middle, low, nothing], 1
            ).astype(BF16)


def x_pack(index, queries, output_grad, output, logs):
    shape = (2, BLOCK, PACKED)
    return call(
        x_pack_kernel,
        1,
        [whole(a.shape) for a in (queries, output_grad, output, logs)],
        [(whole(shape), jax.ShapeDtypeStruct(shape, BF16))] * 4,
        [],
        3,
    )(index, queries, output_grad, output, logs)


def finish_kernel(index_ref, both_ref, k_ref, v_ref):
    for h in range(HEADS):
        for a in range(2):
            cols = slice(h * HEAD, (h + 1) * HEAD)
            k_ref[0, a, :, cols] = both_ref[h, a, 0]
            v_ref[0, a, :, cols] = both_ref[h, a, 1]


def finish(index, both):
    shape = (1, 2, BLOCK, HEADS * HEAD)
    return call(
        finish_kernel,
        1,
        [whole(both.shape)],
        [(whole(shape), jax.ShapeDtypeStruct(shape, F32))] * 2,
        [],
        1,
    )(index, both)


def place_kernel(index_ref, *refs):
    *ins, out = refs
    y = index_ref[0] // 8
    for p, ref in enumerate(ins):
        at = ((y + STEPS[p]) % 4) * WIDTH
        out[:, :, pl.ds(pl.multiple_of(at, WIDTH), WIDTH)] = ref[...]


def place_queries(index, backs):
    shape = (2, BLOCK, HEADS * WIDTH)
    return call(
        place_kernel,
        1,
        [whole((2, BLOCK, WIDTH))] * 4,
        [(whole(shape), jax.ShapeDtypeStruct(shape, F32))],
        [],
        2,
    )(index, *backs)[0]


def body(queries, keys, values, output, output_grad, logs):
    index = lax.axis_index("seq").astype(jnp.int32)
    send = lambda a, perm: lax.ppermute(a, "seq", perm)

    place = index.reshape(1)
    pieces = list(kv_pack(place, keys, values))
    for p in (1, 2, 3):
        pieces[p] = send(pieces[p], along_y(STEPS[p]))
    kv = jnp.stack(pieces)

    xs = list(x_pack(place, queries, output_grad, output, logs))
    for p in (1, 2, 3):
        xs[p] = send(xs[p], along_y(STEPS[p]))
    slots = [kv]
    for k in (1, 2, 3):
        slots.append(send(kv, along_z(k)))
    kv_own = jnp.stack(slots)
    kv_other = send(kv_own, OTHER_CORE)

    def summed(own, other):
        other = send(other, OTHER_CORE)
        mine = own[0] + other[0]
        for k in (1, 2, 3):
            part = own[k] + other[k]
            part = send(part, along_z(k))
            mine = mine + part
        return mine

    def to_owners(mine):
        return lax.all_to_all(
            mine, "seq", 0, 0, axis_index_groups=Y_GROUPS, tiled=True
        )

    dq_own, kt, vt, dk, dv = own_call(place, xs[0], kv_own, kv_other)
    dq_late, own, other = late_call(place, xs[1:], kt, vt, dk, dv)
    late = summed(own, other)
    dq_12, dk, dv = early_call((1, 2), place, xs, kt, vt, dk, dv, dq_late)
    dq_3, own, other = early_call((3,), place, xs, kt, vt, dk, dv, dq_late)
    early = summed(own, other)
    both = to_owners(jnp.stack([early, late], 1))
    key_gradient, value_gradient = finish(place, both)
    dq = [dq_own, dq_12[0:2], dq_12[2:4], dq_3]

    backs = [dq[0]]
    for p in (1, 2, 3):
        backs.append(send(dq[p], along_y(-STEPS[p])))
    grad_query = place_queries(place, backs)

    return grad_query[None], key_gradient, value_gradient


def solution(mesh):
    placed = P("seq", None, "dp", None)

    return jax.shard_map(
        body,
        mesh=mesh,
        in_specs=(placed,) * 6,
        out_specs=(placed,) * 3,
        check_vma=False,
    )
```

```python
import jax
import jax.numpy as jnp
from jax import lax
from jax.experimental import pallas as pl
from jax.experimental.pallas import tpu as pltpu
from jax.sharding import PartitionSpec as P

HEAD = 128
GROUP = 8
BLOCK = 64
ROWS = GROUP * BLOCK
WIDTH = GROUP * HEAD
HEADS = 4
TILE = 512
VMEM_LIMIT = 28 * 2**20
HALF = 32 * BLOCK
STEPS = (0, 1, 3, 2)
SCALE = HEAD ** -0.5
LOG2E = 1.4426950408889634
F32 = jnp.float32
BF16 = jnp.bfloat16


def along_y(step):
    return [(i, (i + 8 * step) % 32) for i in range(32)]


def along_z(step):
    return [(i, (i // 8) * 8 + (i + 2 * step) % 8) for i in range(32)]


OTHER_CORE = [(i, i ^ 1) for i in range(32)]
Y_GROUPS = [[zc + 8 * y for y in range(4)] for zc in range(8)]


def dot(a, b):
    return jnp.dot(a, b, preferred_element_type=F32)


def split(values):
    high = values.astype(BF16)
    return high, (values - high.astype(F32)).astype(BF16)


def owner_of(index, back):
    y, z, c = index // 8, (index // 2) % 4, index % 2
    return ((y + 4 - back) % 4) * 8 + z * 2 + c


def load_block(x_ref, work):
    q_s, do_s, qt_s, dot_s, log_s, delta_s = work
    for j in range(GROUP):
        q_s[j * BLOCK:(j + 1) * BLOCK, :] = x_ref[0, 0:BLOCK, j * HEAD:(j + 1) * HEAD]
        do_s[j * BLOCK:(j + 1) * BLOCK, :] = x_ref[
            0, 0:BLOCK, WIDTH + j * HEAD:WIDTH + (j + 1) * HEAD
        ]
    qt, dt = q_s[...].T, do_s[...].T
    for at in (0, ROWS):
        qt_s[:, at:at + ROWS] = qt
        dot_s[:, at:at + ROWS] = dt
    aux = x_ref[0, :, 2 * WIDTH:].astype(F32)
    aux = aux[:, 0:16] + aux[:, 16:32] + aux[:, 32:48]
    for j in range(GROUP):
        rows = slice(j * BLOCK, (j + 1) * BLOCK)
        log_s[rows, :] = jnp.broadcast_to(aux[:, j:j + 1] * LOG2E, (BLOCK, HEAD))
        delta_s[rows, :] = jnp.broadcast_to(
            aux[:, GROUP + j:GROUP + j + 1], (BLOCK, HEAD)
        )


def sweep(block, low, high, masked, base, kt_ref, vt_ref, dk_ref, dv_ref, dq_s, work, rel_s):
    q_s, do_s, qt_s, dot_s, log_s, delta_s = work
    repeat = TILE // HEAD

    def tile(t, diagonal):
        at = pl.multiple_of(t * TILE - base, TILE)
        keys = pl.ds(at, TILE)
        kt, vt = kt_ref[:, keys], vt_ref[:, keys]
        scores = dot(q_s[...], kt)
        weight_grad = dot(do_s[...], vt)
        log_b = jnp.concatenate([log_s[...]] * repeat, 1)
        delta_b = jnp.concatenate([delta_s[...]] * repeat, 1)
        weights = jnp.exp2(scores * (SCALE * LOG2E) - log_b)
        if diagonal:
            weights = jnp.where(rel_s[...] <= block * BLOCK - t * TILE, weights, 0.0)
        w_high, w_rest = split(weights)
        s_high, s_rest = split(weights * (weight_grad - delta_b))
        dv_ref[:, keys] += dot(dot_s[...], jnp.concatenate([w_high, w_rest], 0))
        dk_ref[:, keys] += dot(qt_s[...], jnp.concatenate([s_high, s_rest], 0))
        dq_s[...] += dot(
            jnp.concatenate([kt, kt], 1), jnp.concatenate([s_high.T, s_rest.T], 0)
        )

    @pl.loop(low, high)
    def _(t):
        tile(t, False)

    if masked is True:
        tile(high, True)
    elif masked is not False:
        @pl.when(masked)
        def _():
            tile(high, True)


def relative(rel_s):
    shape = (ROWS, TILE)
    rel_s[...] = lax.broadcasted_iota(jnp.int32, shape, 1) - (
        lax.broadcasted_iota(jnp.int32, shape, 0) % BLOCK
    )


def write_queries(dq_s, dq_ref):
    dq = (dq_s[...] * SCALE).T
    for j in range(GROUP):
        dq_ref[0, :, j * HEAD:(j + 1) * HEAD] = dq[j * BLOCK:(j + 1) * BLOCK, :]


def write_slots(index, late, dk_s, dv_s, out_s, own_ref, other_ref):
    z, c = (index // 2) % 4, index % 2
    for kind, acc in ((0, dk_s), (1, dv_s)):
        out_s[...] = (acc[...] * SCALE).T if kind == 0 else acc[...].T
        for ref, core in ((own_ref, c), (other_ref, 1 - c)):
            for k in range(4):
                for s in range(4):
                    n = s * 8 + ((z + k) % 4) * 2 + core
                    row = (31 - n if late else n) * BLOCK
                    rows = pl.ds(pl.multiple_of(row, BLOCK), BLOCK)
                    ref[k, s, kind] = out_s[rows, :]


def own_kernel(
    index_ref, x_ref, kv_own, kv_other, dq_ref, kt_ref, vt_ref, dk_ref, dv_ref,
    *scratch,
):
    k_s, v_s, dq_s, rel_s, *work = scratch
    half = pl.program_id(0)
    index = index_ref[0]
    y, z, c = index // 8, (index // 2) % 4, index % 2
    owner = owner_of(index, 0)
    block = jnp.where(half == 0, owner, 63 - owner)

    @pl.when(half == 0)
    def _():
        relative(rel_s)
        dk_ref[...] = jnp.zeros_like(dk_ref)
        dv_ref[...] = jnp.zeros_like(dv_ref)
        for ref, core in ((kv_own, c), (kv_other, 1 - c)):
            for k in range(4):
                for s in range(4):
                    n = ((y + 4 - STEPS[s]) % 4) * 8 + ((z - k + 4) % 4) * 2 + core
                    for a in range(2):
                        row = (n if a == 0 else 63 - n) * BLOCK
                        rows = pl.ds(pl.multiple_of(row, BLOCK), BLOCK)
                        k_s[rows, :] = ref[k, s, 0, a]
                        v_s[rows, :] = ref[k, s, 1, a]
        kt_ref[...] = k_s[...].T
        vt_ref[...] = v_s[...].T

    load_block(x_ref, work)
    dq_s[...] = jnp.zeros_like(dq_s)
    full = block // (TILE // BLOCK)
    sweep(block, 0, full, True, 0, kt_ref, vt_ref, dk_ref, dv_ref, dq_s, work, rel_s)
    write_queries(dq_s, dq_ref)


def late_kernel(
    index_ref, x1, x2, x3, kt_ref, vt_ref, dk_in, dv_in, dq_ref, own_ref, other_ref,
    *scratch,
):
    dk_s, dv_s, out_s, dq_s, rel_s, *work = scratch
    step = pl.program_id(0)
    index = index_ref[0]

    @pl.when(step == 0)
    def _():
        relative(rel_s)
        dk_s[...] = dk_in[...]
        dv_s[...] = dv_in[...]

    for p, x_ref in enumerate((x1, x2, x3)):
        pl.when(step == p)(lambda x_ref=x_ref: load_block(x_ref, work))
    back = jnp.where(step == 0, STEPS[1], jnp.where(step == 1, STEPS[2], STEPS[3]))
    block = 63 - owner_of(index, back)
    dq_s[...] = jnp.zeros_like(dq_s)
    full = block // (TILE // BLOCK)
    sweep(
        block, HALF // TILE, full, True, HALF, kt_ref, vt_ref, dk_s, dv_s, dq_s, work,
        rel_s,
    )
    dq_ref[0] = dq_s[...]

    @pl.when(step == 2)
    def _():
        write_slots(index, True, dk_s, dv_s, out_s, own_ref, other_ref)


def early_kernel(pairs, last, index_ref, *refs):
    count = len(pairs)
    x_refs, refs = refs[:count], refs[count:]
    kt_ref, vt_ref, dk_in, dv_in, dq_in, dq_ref, *rest = refs
    if last:
        own_ref, other_ref, dk_s, dv_s, out_s, dq_s, rel_s, *work = rest
    else:
        dk_s, dv_s, dq_s, rel_s, *work = rest
    step = pl.program_id(0)
    index = index_ref[0]
    back = STEPS[pairs[0]]
    if count == 2:
        back = jnp.where(step < 2, back, STEPS[pairs[1]])
    owner = owner_of(index, back)
    first = step % 2 == 0
    block = jnp.where(first, 63 - owner, owner)

    @pl.when(step == 0)
    def _():
        relative(rel_s)
        dk_s[...] = dk_in[...]
        dv_s[...] = dv_in[...]

    @pl.when(first)
    def _():
        dq_s[...] = dq_in[0]

    @pl.when(step % 2 == 1)
    def _():
        dq_s[...] = jnp.zeros_like(dq_s)

    if count == 1:
        load_block(x_refs[0], work)
    else:
        for p, x_ref in enumerate(x_refs):
            pl.when(step // 2 == p)(lambda x_ref=x_ref: load_block(x_ref, work))
    full = jnp.minimum(block // (TILE // BLOCK), HALF // TILE)
    sweep(
        block, 0, full, step % 2 == 1, 0, kt_ref, vt_ref, dk_s, dv_s, dq_s, work, rel_s
    )
    write_queries(dq_s, dq_ref)

    if last:
        @pl.when(step == 2 * count - 1)
        def _():
            write_slots(index, False, dk_s, dv_s, out_s, own_ref, other_ref)


WORK = [
    pltpu.VMEM((HEAD, ROWS), F32),
    pltpu.VMEM((ROWS, TILE), jnp.int32),
    pltpu.VMEM((ROWS, HEAD), BF16),
    pltpu.VMEM((ROWS, HEAD), BF16),
    pltpu.VMEM((HEAD, 2 * ROWS), BF16),
    pltpu.VMEM((HEAD, 2 * ROWS), BF16),
    pltpu.VMEM((ROWS, HEAD), F32),
    pltpu.VMEM((ROWS, HEAD), F32),
]
PACKED = 2 * WIDTH + HEAD
X_BLOCK = (1, BLOCK, PACKED)
SLOTS = (4, 4, 2, BLOCK, HEAD)


def whole(shape):
    return pl.BlockSpec(shape, lambda i, p: (0,) * len(shape))


def half_of(which):
    return pl.BlockSpec((HEAD, HALF), lambda i, p: (0, which))


def call(kernel, steps, ins, outs, scratch, micros):
    return pl.pallas_call(
        kernel,
        grid_spec=pltpu.PrefetchScalarGridSpec(
            num_scalar_prefetch=1,
            grid=(steps,),
            in_specs=ins,
            out_specs=[spec for spec, _ in outs],
            scratch_shapes=scratch,
        ),
        out_shape=[shape for _, shape in outs],
        compiler_params=pltpu.CompilerParams(
            dimension_semantics=("arbitrary",), vmem_limit_bytes=VMEM_LIMIT
        ),
        cost_estimate=pl.CostEstimate(
            flops=int(micros * 5e8), transcendentals=0, bytes_accessed=8 * 2**20
        ),
    )


DQ_BLOCK = (1, BLOCK, WIDTH)


def own_call(index, x, kv_own, kv_other):
    keys = 2 * HALF
    kv_shape = (4, 4, 2, 2, BLOCK, HEAD)
    return call(
        own_kernel,
        2,
        [pl.BlockSpec(X_BLOCK, lambda i, p: (i, 0, 0)), whole(kv_shape), whole(kv_shape)],
        [
            (
                pl.BlockSpec(DQ_BLOCK, lambda i, p: (i, 0, 0)),
                jax.ShapeDtypeStruct((2, BLOCK, WIDTH), F32),
            ),
            (whole((HEAD, keys)), jax.ShapeDtypeStruct((HEAD, keys), BF16)),
            (whole((HEAD, keys)), jax.ShapeDtypeStruct((HEAD, keys), BF16)),
            (whole((HEAD, keys)), jax.ShapeDtypeStruct((HEAD, keys), F32)),
            (whole((HEAD, keys)), jax.ShapeDtypeStruct((HEAD, keys), F32)),
        ],
        [pltpu.VMEM((keys, HEAD), BF16)] * 2 + WORK,
        13,
    )(index, x, kv_own, kv_other)


SLOT_OUTS = [(whole(SLOTS), jax.ShapeDtypeStruct(SLOTS, F32))] * 2
ACCUMULATORS = [pltpu.VMEM((HEAD, HALF), F32)] * 2
TURNED = [pltpu.VMEM((HALF, HEAD), F32)]


def late_call(index, xs, kt, vt, dk, dv):
    return call(
        late_kernel,
        3,
        [pl.BlockSpec(X_BLOCK, lambda i, p: (1, 0, 0))] * 3 + [half_of(1)] * 4,
        [
            (
                pl.BlockSpec((1, HEAD, ROWS), lambda i, p: (i, 0, 0)),
                jax.ShapeDtypeStruct((3, HEAD, ROWS), F32),
            )
        ] + SLOT_OUTS,
        ACCUMULATORS + TURNED + WORK,
        10,
    )(index, *xs, kt, vt, dk, dv)


def early_call(pairs, index, xs, kt, vt, dk, dv, dq):
    count, last = len(pairs), pairs[-1] == 3
    acc = [(whole((HEAD, HALF)), jax.ShapeDtypeStruct((HEAD, HALF), F32))] * 2
    return call(
        lambda *refs: early_kernel(pairs, last, *refs),
        2 * count,
        [pl.BlockSpec(X_BLOCK, lambda i, p: (1 - i % 2, 0, 0))] * count
        + [half_of(0)] * 4
        + [pl.BlockSpec((1, HEAD, ROWS), lambda i, p: (pairs[0] - 1 + i // 2, 0, 0))],
        [
            (
                pl.BlockSpec(DQ_BLOCK, lambda i, p: ((i // 2) * 2 + 1 - i % 2, 0, 0)),
                jax.ShapeDtypeStruct((2 * count, BLOCK, WIDTH), F32),
            )
        ] + (SLOT_OUTS if last else acc),
        (ACCUMULATORS + TURNED if last else []) + WORK,
        9 * count,
    )(index, *[xs[p] for p in pairs], kt, vt, dk, dv, dq)


def kv_pack_kernel(index_ref, k_ref, v_ref, *outs):
    y = index_ref[0] // 8
    for p, out in enumerate(outs):
        at = pl.multiple_of(((y + STEPS[p]) % 4) * HEAD, HEAD)
        out[0] = k_ref[0, :, :, pl.ds(at, HEAD)]
        out[1] = v_ref[0, :, :, pl.ds(at, HEAD)]


def kv_pack(index, keys, values):
    shape = (2, 2, BLOCK, HEAD)
    return call(
        kv_pack_kernel,
        1,
        [whole(keys.shape)] * 2,
        [(whole(shape), jax.ShapeDtypeStruct(shape, BF16))] * 4,
        [],
        1,
    )(index, keys, values)


def x_pack_kernel(slots, index_ref, q_ref, d_ref, o_ref, log_ref, *outs):
    y = index_ref[0] // 8
    for p, out in zip(slots, outs):
        head = (y + STEPS[p]) % 4
        at = pl.multiple_of(head * WIDTH, WIDTH)
        for a in range(2):
            q = q_ref[0, a, :, pl.ds(at, WIDTH)]
            d = d_ref[0, a, :, pl.ds(at, WIDTH)]
            o = o_ref[0, a, :, pl.ds(at, WIDTH)]
            out[a, :, 0:WIDTH] = q
            out[a, :, WIDTH:2 * WIDTH] = d
            product = d.astype(F32) * o.astype(F32)
            logs = log_ref[0, a]
            mine = logs[:, 0:GROUP]
            for h in range(1, HEADS):
                mine = jnp.where(head == h, logs[:, h * GROUP:(h + 1) * GROUP], mine)
            rows = jnp.concatenate(
                [mine]
                + [
                    jnp.sum(product[:, j * HEAD:(j + 1) * HEAD], 1, keepdims=True)
                    for j in range(GROUP)
                ],
                1,
            )
            high = rows.astype(BF16).astype(F32)
            middle = (rows - high).astype(BF16).astype(F32)
            low = rows - high - middle
            nothing = jnp.zeros((BLOCK, HEAD - 48), F32)
            out[a, :, 2 * WIDTH:] = jnp.concatenate(
                [high, middle, low, nothing], 1
            ).astype(BF16)


def x_pack(slots, index, queries, output_grad, output, logs):
    shape = (2, BLOCK, PACKED)
    return call(
        lambda *refs: x_pack_kernel(slots, *refs),
        1,
        [whole(a.shape) for a in (queries, output_grad, output, logs)],
        [(whole(shape), jax.ShapeDtypeStruct(shape, BF16))] * len(slots),
        [],
        3,
    )(index, queries, output_grad, output, logs)


def finish_kernel(index_ref, both_ref, k_ref, v_ref):
    for h in range(HEADS):
        for a in range(2):
            cols = slice(h * HEAD, (h + 1) * HEAD)
            k_ref[0, a, :, cols] = both_ref[h, a, 0]
            v_ref[0, a, :, cols] = both_ref[h, a, 1]


def finish(index, both):
    shape = (1, 2, BLOCK, HEADS * HEAD)
    return call(
        finish_kernel,
        1,
        [whole(both.shape)],
        [(whole(shape), jax.ShapeDtypeStruct(shape, F32))] * 2,
        [],
        1,
    )(index, both)


def place_kernel(index_ref, *refs):
    *ins, out = refs
    y = index_ref[0] // 8
    for p, ref in enumerate(ins):
        at = ((y + STEPS[p]) % 4) * WIDTH
        out[:, :, pl.ds(pl.multiple_of(at, WIDTH), WIDTH)] = ref[...]


def place_queries(index, backs):
    shape = (2, BLOCK, HEADS * WIDTH)
    return call(
        place_kernel,
        1,
        [whole((2, BLOCK, WIDTH))] * 4,
        [(whole(shape), jax.ShapeDtypeStruct(shape, F32))],
        [],
        2,
    )(index, *backs)[0]


def body(queries, keys, values, output, output_grad, logs):
    index = lax.axis_index("seq").astype(jnp.int32)
    send = lambda a, perm: lax.ppermute(a, "seq", perm)

    place = index.reshape(1)
    pieces = list(kv_pack(place, keys, values))
    for p in (1, 2, 3):
        pieces[p] = send(pieces[p], along_y(STEPS[p]))
    kv = jnp.stack(pieces)

    rows = (queries, output_grad, output, logs)
    sent = x_pack((1, 2, 3), place, *rows)
    xs = [*x_pack((0,), place, *rows), *sent]
    for p in (1, 2, 3):
        xs[p] = send(xs[p], along_y(STEPS[p]))
    slots = [kv]
    for k in (1, 2, 3):
        slots.append(send(kv, along_z(k)))
    kv_own = jnp.stack(slots)
    kv_other = send(kv_own, OTHER_CORE)

    def summed(own, other):
        other = send(other, OTHER_CORE)
        mine = own[0] + other[0]
        for k in (1, 2, 3):
            part = own[k] + other[k]
            part = send(part, along_z(k))
            mine = mine + part
        return mine

    def to_owners(mine):
        return lax.all_to_all(
            mine, "seq", 0, 0, axis_index_groups=Y_GROUPS, tiled=True
        )

    dq_own, kt, vt, dk, dv = own_call(place, xs[0], kv_own, kv_other)
    dq_late, own, other = late_call(place, xs[1:], kt, vt, dk, dv)
    late = summed(own, other)
    dq_12, dk, dv = early_call((1, 2), place, xs, kt, vt, dk, dv, dq_late)
    dq_3, own, other = early_call((3,), place, xs, kt, vt, dk, dv, dq_late)
    early = summed(own, other)
    both = to_owners(jnp.stack([early, late], 1))
    key_gradient, value_gradient = finish(place, both)
    dq = [dq_own, dq_12[0:2], dq_12[2:4], dq_3]

    backs = [dq[0]]
    for p in (1, 2, 3):
        backs.append(send(dq[p], along_y(-STEPS[p])))
    grad_query = place_queries(place, backs)

    return grad_query[None], key_gradient, value_gradient


def solution(mesh):
    placed = P("seq", None, "dp", None)

    return jax.shard_map(
        body,
        mesh=mesh,
        in_specs=(placed,) * 6,
        out_specs=(placed,) * 3,
        check_vma=False,
    )
```
